32 devices in a mesh: member: 4 (over y, core), node: 8 (over z, x).
Axes of the slice: x: 2, y: 2, z: 4, core: 2. Of those that a mesh axis runs over, the one named last changes fastest.
Arguments:
- gridpoint_state: bfloat16 [218, 8192], P(None, 'node'), may hold values from -6 to 6
- grid_truth: bfloat16 [100, 8192], P(None, 'node'), may hold values from -6 to 6
- encoder_slots: int32 [2048, 16], P('node'), may hold values from 0 to 8191, as said below
- encoder_count: int32 [2048], P('node'), may hold values from 1 to 16
- node_reach: int32 [2048], P('node'), may hold values from 128 to 256
- decoder_slots: int32 [8192, 4], P('node'), may hold values from 0 to 2047, as said below
- member_perturb: bfloat16 [4, 2048, 1024], P('member', 'node'), may hold values from -6 to 6
- embed_weight: bfloat16 [218, 1024], replicated, may hold values from -0.4375 to 0.4375
- norm_gains: float32 [3, 1024], replicated, may hold values from 0.1 to 1.9
- qkv_weight: bfloat16 [1024, 3072], replicated
- out_weight: bfloat16 [1024, 1024], replicated, may hold values from -0.1875 to 0.1875
- up_weight: bfloat16 [1024, 4096], P('node'), may hold values from -0.1875 to 0.1875
- down_weight: bfloat16 [1024, 4096], P('node'), may hold values from -0.09375 to 0.09375
- head_weight: bfloat16 [1024, 100], replicated, may hold values from -0.1875 to 0.1875
Outputs:
- crps_grad: float32 [4, 100, 8192], P('member', None, 'node')
The draws below stay inside these ranges and needn't reach their ends.
Inputs may be any that keep to these rules, and one draw needn't show every extreme that they name: `encoder_slots`: for a hidden node of region r (nodes r * 256 to (r + 1) * 256 - 1), every slot names a grid point of region r - 1, r or r + 1, a region holding 1024 consecutive points; slots from encoder_count on are padding. `decoder_slots`: for a grid point of region r, every slot names a hidden node of region r - 1, r or r + 1.
All inputs are finite; a program needn't handle non-finite values.
Results may differ from the reference program's by a relative error of at most 0.0095.
The reference program's roundings to bfloat16 on the way count: a program that leaves them out, or rounds other values in their place, can miss the bound.
Values may be sent and summed in bfloat16 or wider, within the bound.
A program may use at most 128 MiB of HBM per device.

```python
import jax
import jax.numpy as jnp
from jax import lax

D = 1024
HEADS = 16
HEAD_DIM = 64
FF = 4096
CH = 218
VARS = 100
BAND = 256
K_ENC = 16
K_DEC = 4
NODE_DEV = 256
GRID_DEV = 1024
NODES = 2048
POINTS = 8192
MEMBERS = 4


def window_slots(key, row_count, per_region, target_region, target_total, slot_count):
    region_count = target_total // target_region
    owners = jnp.arange(row_count, dtype=jnp.int32) // per_region
    lowest = jnp.maximum(owners - 1, 0) * target_region
    highest = jnp.minimum(owners + 2, region_count) * target_region
    drawn = jax.random.randint(key, (row_count, slot_count), 0, 3 * target_region, dtype=jnp.int32)
    return lowest[:, None] + drawn % (highest - lowest)[:, None]


def draw_encoder_slots(key, part):
    return window_slots(jax.random.fold_in(key, 11), NODES, NODE_DEV, GRID_DEV, POINTS, K_ENC)


def draw_decoder_slots(key, part):
    return window_slots(jax.random.fold_in(key, 23), POINTS, GRID_DEV, NODE_DEV, NODES, K_DEC)


def draw_qkv_weight(key, part):
    entries = jax.random.normal(jax.random.fold_in(key, 37), (D, 3 * D), jnp.float32) * D ** (-0.5)
    return entries.astype(jnp.bfloat16)


def touch_ends(array, rng, low, largest):
    spot = [jax.random.randint(jax.random.fold_in(rng, axis), (), 0, length) for axis, length in enumerate(array.shape)]
    widest = array.shape.index(max(array.shape))
    neighbour = spot[:widest] + [(spot[widest] + 1) % array.shape[widest]] + spot[widest + 1:]
    return array.at[tuple(spot)].set(low).at[tuple(neighbour)].set(largest)


def block_scale(own_key, shape, split, smallest, largest):
    def one(axis_at, shards_of):
        draws = jax.random.uniform(jax.random.fold_in(jax.random.fold_in(own_key, 6), axis_at), (shards_of,), jnp.float32, smallest / len(split), largest / len(split))
        return jnp.repeat(jnp.exp(draws), shape[axis_at] // shards_of).reshape((-1,) + (1,) * (len(shape) - axis_at - 1))

    factor_of = one(*split[0])
    for cut in split[1:]:
        factor_of = factor_of * one(*cut)
    return factor_of


def scatter_about(own_key, extent, deviation, reach, cuts=(), kind=jnp.bfloat16):
    values = deviation * jax.random.normal(own_key, extent, jnp.float32)
    if cuts:
        values = values * block_scale(own_key, extent, cuts, -0.22, 0.18)
    return jnp.clip(values, -reach, reach).astype(kind)


def setup_inputs(seed: int = 0) -> dict:
    keys = jax.random.split(jax.random.key(seed), 15)
    gridpoint_state = scatter_about(keys[0], (CH, POINTS), 1.0, 6.0, ((1, 8),))
    grid_truth = scatter_about(keys[1], (VARS, POINTS), 1.0, 6.0, ((1, 8),))
    encoder_slots = draw_encoder_slots(jax.random.fold_in(keys[14], 71), 0)
    encoder_count = touch_ends(jax.random.randint(keys[3], (NODES,), 1, K_ENC + 1), jax.random.fold_in(keys[3], 1), 1, K_ENC).astype(jnp.int32)
    node_reach = touch_ends(jax.random.randint(keys[4], (NODES,), BAND // 2, BAND + 1), jax.random.fold_in(keys[4], 1), BAND // 2, BAND).astype(jnp.int32)
    decoder_slots = draw_decoder_slots(jax.random.fold_in(keys[14], 71), 0)
    member_perturb = scatter_about(keys[6], (MEMBERS, NODES, D), 1.0, 6.0, ((0, 4), (1, 8)))
    embed_weight = scatter_about(keys[7], (CH, D), CH ** -0.5, 0.4375)
    norm_gains = jnp.clip(1.0 + 0.18 * jax.random.normal(keys[8], (3, D), jnp.float32), 0.1, 1.9)
    qkv_weight = draw_qkv_weight(jax.random.fold_in(keys[14], 71), 0)
    out_weight = scatter_about(keys[10], (D, D), D ** -0.5, 0.1875)
    up_weight = scatter_about(keys[11], (D, FF), D ** -0.5, 0.1875, ((0, 8),))
    down_weight = scatter_about(keys[12], (D, FF), FF ** -0.5, 0.09375, ((0, 8),))
    head_weight = scatter_about(keys[13], (D, VARS), D ** -0.5, 0.1875)
    return dict(gridpoint_state=gridpoint_state, grid_truth=grid_truth, encoder_slots=encoder_slots, encoder_count=encoder_count, node_reach=node_reach, decoder_slots=decoder_slots, member_perturb=member_perturb, embed_weight=embed_weight, norm_gains=norm_gains, qkv_weight=qkv_weight, out_weight=out_weight, up_weight=up_weight, down_weight=down_weight, head_weight=head_weight)


EPS = 1e-05
SMOOTH = 0.25

def layer_norm(entries, scale_gain):
    average = lax.optimization_barrier(jnp.mean(entries, axis=-1, keepdims=True))
    centred = entries - average
    variance = lax.optimization_barrier(jnp.mean(centred * centred, axis=-1, keepdims=True))
    return centred * lax.rsqrt(variance + EPS) * scale_gain

def score_gradient(difference):
    return difference * lax.rsqrt(difference * difference + SMOOTH * SMOOTH)

def banded_attention(query_rows, bordered, first_query, first_key, node_total, reaches):
    query_count = query_rows.shape[0]
    key_count = bordered.shape[0]
    model_width = query_rows.shape[1]
    key_heads = bordered[:, :model_width].reshape(key_count, HEADS, HEAD_DIM).astype(jnp.float32)
    value_heads = bordered[:, model_width:].reshape(key_count, HEADS, HEAD_DIM).astype(jnp.float32)
    queries = query_rows.reshape(query_count, HEADS, HEAD_DIM).astype(jnp.float32)
    scores = jnp.einsum('qhd,khd->hqk', queries, key_heads) * HEAD_DIM ** (-0.5)
    rows_at = first_query + jnp.arange(query_count, dtype=jnp.int32)
    cols_at = first_key + jnp.arange(key_count, dtype=jnp.int32)
    distance = jnp.abs(rows_at[:, None] - cols_at[None, :])
    allowed = (distance <= reaches[:, None]) & (cols_at[None, :] >= 0) & (cols_at[None, :] < node_total)
    masked = jnp.where(allowed[None], scores, -1e+30)
    highest = lax.optimization_barrier(jnp.max(masked, axis=-1, keepdims=True))
    weights = jnp.where(allowed[None], jnp.exp(masked - highest), 0.0)
    chances = (weights / lax.optimization_barrier(jnp.sum(weights, axis=-1, keepdims=True))).astype(jnp.bfloat16)
    blended = jnp.einsum('hqk,khd->qhd', chances.astype(jnp.float32), value_heads)
    return blended.reshape(query_count, model_width).astype(jnp.bfloat16)

def reference(gridpoint_state, grid_truth, encoder_slots, encoder_count, node_reach, decoder_slots, member_perturb, embed_weight, norm_gains, qkv_weight, out_weight, up_weight, down_weight, head_weight):
    columns = gridpoint_state.T
    used = (jnp.arange(K_ENC, dtype=jnp.int32)[None, :] < encoder_count[:, None]).astype(jnp.float32)
    pooled_sum = jnp.zeros((NODES, CH), jnp.float32)
    for position in range(K_ENC):
        picked = jnp.take(columns, encoder_slots[:, position], axis=0).astype(jnp.float32)
        pooled_sum = pooled_sum + picked * used[:, position:position + 1]
    pooled_nodes = (pooled_sum / encoder_count[:, None].astype(jnp.float32)).astype(jnp.bfloat16)
    embedded = jnp.dot(pooled_nodes, embed_weight, preferred_element_type=jnp.float32)
    head_wide = head_weight.astype(jnp.float32)

    def member_prediction(perturb_rows):
        hidden_start = embedded + perturb_rows.astype(jnp.float32)
        normed = layer_norm(hidden_start, norm_gains[0]).astype(jnp.bfloat16)
        project = jnp.dot(normed, qkv_weight, preferred_element_type=jnp.float32).astype(jnp.bfloat16)
        query_all = project[:, :D]
        padded = jnp.pad(project[:, D:], ((BAND, BAND), (0, 0)))

        def one_block(block):
            first = (block * NODE_DEV).astype(jnp.int32)
            query_rows = lax.dynamic_slice_in_dim(query_all, first, NODE_DEV, 0)
            bordered = lax.dynamic_slice_in_dim(padded, first, NODE_DEV + 2 * BAND, 0)
            reaches = lax.dynamic_slice_in_dim(node_reach, first, NODE_DEV, 0)
            return banded_attention(query_rows, bordered, first, first - BAND, NODES, reaches)
        attended = lax.map(one_block, jnp.arange(NODES // NODE_DEV, dtype=jnp.int32)).reshape(NODES, D)
        hidden_mid = hidden_start + jnp.dot(attended, out_weight, preferred_element_type=jnp.float32)
        normed_mid = layer_norm(hidden_mid, norm_gains[1]).astype(jnp.bfloat16)
        upper = jnp.dot(normed_mid, up_weight, preferred_element_type=jnp.float32)
        active = jax.nn.gelu(upper).astype(jnp.bfloat16)
        lowered = lax.dot_general(active, down_weight, (((1,), (1,)), ((), ())), preferred_element_type=jnp.float32)
        final = layer_norm(hidden_mid + lowered, norm_gains[2]).astype(jnp.bfloat16)
        summed = jnp.zeros((POINTS, D), jnp.float32)
        for position in range(K_DEC):
            summed = summed + jnp.take(final, decoder_slots[:, position], axis=0).astype(jnp.float32)
        gathered = summed / K_DEC
        state_delta = lax.dot_general(head_wide, gathered, (((0,), (1,)), ((), ())), precision=lax.Precision.HIGHEST, preferred_element_type=jnp.float32)
        return gridpoint_state[:VARS].astype(jnp.float32) + state_delta
    predicted_fields = lax.map(member_prediction, member_perturb)
    observed_field = grid_truth.astype(jnp.float32)
    gradients = []
    for member_index in range(MEMBERS):
        self_field = predicted_fields[member_index]
        pairwise_sum = jnp.zeros_like(self_field)
        for other_member in range(MEMBERS):
            pairwise_sum = pairwise_sum + score_gradient(self_field - predicted_fields[other_member])
        gradients.append(score_gradient(self_field - observed_field) / MEMBERS - pairwise_sum / (MEMBERS * (MEMBERS - 1)))
    return jnp.stack(gradients)
```

```python
import functools

import jax
import jax.numpy as jnp
from jax import lax
from jax.experimental import pallas as pl
from jax.experimental.pallas import tpu as pltpu
from jax.sharding import PartitionSpec as P

HEAD_DIM = 64

EPS = 1e-05
SMOOTH = 0.25


def halo_parts(block, dim, width):
    count = lax.axis_size("node")
    forward = [(i, i + 1) for i in range(count - 1)]
    backward = [(target, source) for source, target in forward]
    low = lax.ppermute(
        lax.slice_in_dim(block, block.shape[dim] - width, None, axis=dim), "node", forward
    )
    high = lax.ppermute(lax.slice_in_dim(block, 0, width, axis=dim), "node", backward)
    return low, high


def with_halo(block, dim, width):
    low, high = halo_parts(block, dim, width)
    return jnp.concatenate([low, block, high], axis=dim)


def layer_norm(entries, scale_gain):
    average = jnp.mean(entries, axis=-1, keepdims=True)
    centred = entries - average
    variance = jnp.mean(centred * centred, axis=-1, keepdims=True)
    return centred * lax.rsqrt(variance + EPS) * scale_gain


def score_gradient(difference):
    return difference * lax.rsqrt(difference * difference + SMOOTH * SMOOTH)


def times_rows(left_side, right_side):
    return lax.dot_general(
        left_side, right_side, (((1,), (1,)), ((), ())), preferred_element_type=jnp.float32
    )


def count_slots(local_slots, live, width):
    window = jnp.arange(width, dtype=jnp.int32)
    tallies = jnp.zeros((local_slots.shape[0], width), jnp.float32)
    for position in range(local_slots.shape[1]):
        hits = local_slots[:, position][:, None] == window[None, :]
        if live is not None:
            hits = hits & live(position)[:, None]
        tallies = tallies + hits.astype(jnp.float32)
    return lax.optimization_barrier(tallies.astype(jnp.bfloat16))


def copy_to(source, target, send_sem, recv_sem, **place):
    return pltpu.make_async_remote_copy(
        src_ref=source,
        dst_ref=target,
        send_sem=send_sem,
        recv_sem=recv_sem,
        device_id=place,
        device_id_type=pl.DeviceIdType.MESH,
    )


def signal(**place):
    pl.semaphore_signal(
        pltpu.get_barrier_semaphore(),
        inc=1,
        device_id=place,
        device_id_type=pl.DeviceIdType.MESH,
    )


def ring_place(region, count):
    odd = lax.rem(region, 2)
    half = lax.div(region, 2)
    return (1 - odd) * half + odd * (count - 1 - half)


def ring_region(place, count):
    late = lax.div(place, count // 2)
    return (1 - late) * 2 * place + late * (2 * (count - 1 - place) + 1)


class WeightRing:
    def __init__(self, count, member, parts, wholes, send_sems, recv_sems, own_sems):
        region = lax.axis_index("node")
        place = ring_place(region, count)
        self.hops = (count - 1 - (count - 1) // 2, (count - 1) // 2)
        self.near = (
            ring_region(lax.rem(place + count - 1, count), count),
            ring_region(lax.rem(place + 1, count), count),
        )
        self.waited = set()
        self.copies = {}
        self.own = []
        for which, (part, whole) in enumerate(zip(parts, wholes)):
            rows = whole.shape[0] // count
            width = whole.shape[1]
            mine = part.at[:, pl.ds(pl.multiple_of(member * width, width), width)]
            self.own.append(
                pltpu.make_async_copy(mine, self.slot(whole, region, rows), own_sems.at[which])
            )
            for way in range(2):
                for hop in range(self.hops[way]):
                    shift = hop if way == 0 else count - hop
                    owner = ring_region(lax.rem(place + shift, count), count)
                    there = self.slot(whole, owner, rows)
                    self.copies[which, way, hop] = copy_to(
                        mine if hop == 0 else there,
                        there,
                        send_sems.at[which, way, hop],
                        recv_sems.at[which, way, hop],
                        node=self.near[way],
                    )

    def slot(self, whole, owner, rows):
        return whole.at[pl.ds(pl.multiple_of(owner * rows, rows), rows)]

    def tick(self, which, hop):
        for way in range(2):
            if hop > 0 and (which, way, hop - 1) in self.copies:
                self.copies[which, way, hop - 1].wait_recv()
                self.waited.add((which, way, hop - 1))
            if (which, way, hop) in self.copies:
                self.copies[which, way, hop].start()

    def stage(self, index, stages):
        for hop in range(index * self.hops[0] // stages, (index + 1) * self.hops[0] // stages):
            for which in range(2):
                self.tick(which, hop)

    def finish(self):
        for copy in self.own:
            copy.wait()
        for name, copy in self.copies.items():
            if name not in self.waited:
                copy.wait_recv()
            copy.wait_send()


def front_kernel(
    count, size,
    share_ref, slots_ref, uses_ref, reach_ref, embed_ref, gains_ref, perturb_ref, qkv_ref, out_ref,
    up_ref, down_ref,
    up_out, down_out, mid_out, norm_out,
    state, tallies, pooled, perturb, embed, normed, qkv_w, out_w, query, keys, values_t, bias,
    attended_t, sems, halo_s, halo_r, ring_s, ring_r,
):
    region = lax.axis_index("node")
    member = lax.axis_index("member")
    share, grid_dev = share_ref.shape
    rows = reach_ref.shape[1]
    width = perturb_ref.shape[1]
    node_total = rows * count
    has_low = region > 0
    has_high = region < count - 1
    low = lax.rem(region + count - 1, count)
    high = lax.rem(region + 1, count)
    others = [lax.rem(member + k, size) for k in range(1, size)]
    ring = WeightRing(
        count, member, (up_ref, down_ref), (up_out, down_out), ring_s, ring_r, sems.at[pl.ds(0, 2)]
    )
    own_perturb = pltpu.make_async_copy(perturb_ref, perturb.at[pl.ds(0, rows)], sems.at[2])
    load_qkv = pltpu.make_async_copy(qkv_ref, qkv_w, sems.at[3])
    load_out = pltpu.make_async_copy(out_ref, out_w, sems.at[4])

    @pl.when(jnp.logical_not(has_low))
    def _():
        state[:, 0:grid_dev] = jnp.zeros((share, grid_dev), state.dtype)
        pooled[:, rows : 2 * rows] = jnp.zeros((size * share, rows), pooled.dtype)
        perturb[rows : 2 * rows, :] = jnp.zeros((rows, width), perturb.dtype)

    @pl.when(jnp.logical_not(has_high))
    def _():
        state[:, 2 * grid_dev :] = jnp.zeros((share, grid_dev), state.dtype)
        pooled[:, 2 * rows :] = jnp.zeros((size * share, rows), pooled.dtype)
        perturb[2 * rows :, :] = jnp.zeros((rows, width), perturb.dtype)

    for other in others:
        signal(member=other)
    for near in (low, high, ring.near[0], ring.near[1]):
        signal(node=near)
    pl.semaphore_wait(pltpu.get_barrier_semaphore(), size + 3)

    mine = pl.ds(pl.multiple_of(member * share, share), share)

    def halo(index, source, to_high, to_low):
        up = copy_to(source, to_high, halo_s.at[index, 0], halo_r.at[index, 0], node=high)
        down = copy_to(source, to_low, halo_s.at[index, 1], halo_r.at[index, 1], node=low)
        return up, down

    def start_halo(pair):
        @pl.when(has_high)
        def _():
            pair[0].start()

        @pl.when(has_low)
        def _():
            pair[1].start()

    def take_halo(pair):
        @pl.when(has_low)
        def _():
            pair[0].wait_recv()

        @pl.when(has_high)
        def _():
            pair[1].wait_recv()

    def end_halo(pair):
        @pl.when(has_high)
        def _():
            pair[0].wait_send()

        @pl.when(has_low)
        def _():
            pair[1].wait_send()

    state_halo = halo(
        0, share_ref, state.at[:, pl.ds(0, grid_dev)], state.at[:, pl.ds(2 * grid_dev, grid_dev)]
    )
    perturb_halo = halo(
        1, perturb_ref, perturb.at[pl.ds(rows, rows)], perturb.at[pl.ds(2 * rows, rows)]
    )
    own_pooled = pooled.at[mine, pl.ds(0, rows)]
    pooled_halo = halo(
        2, own_pooled, pooled.at[mine, pl.ds(rows, rows)], pooled.at[mine, pl.ds(2 * rows, rows)]
    )
    start_halo(state_halo)
    start_halo(perturb_halo)
    own_perturb.start()
    load_qkv.start()
    load_out.start()
    for copy in ring.own:
        copy.start()

    state[:, grid_dev : 2 * grid_dev] = share_ref[...]
    embed[...] = jnp.zeros_like(embed)
    embed[0 : embed_ref.shape[0], :] = embed_ref[...]

    tall = 64

    def count_tile(tile, carry):
        base = pl.multiple_of(tile * tall, tall)
        window = lax.broadcasted_iota(jnp.int32, (tall, rows), 0) + base
        total = jnp.zeros((tall, rows), jnp.float32)
        for position in range(slots_ref.shape[0]):
            hits = window == slots_ref[position : position + 1, :]
            total = total + jnp.where(hits, 1.0, 0.0)
        tallies[pl.ds(base, tall), :] = total.astype(jnp.bfloat16)
        return carry

    lax.fori_loop(0, 3 * grid_dev // tall, count_tile, 0)

    take_halo(state_halo)
    pooled_sum = jnp.dot(state[...], tallies[...], preferred_element_type=jnp.float32)
    pooled[mine, 0:rows] = (pooled_sum / uses_ref[...]).astype(jnp.bfloat16)
    pooled_own = [
        copy_to(own_pooled, own_pooled, sems.at[5 + k], sems.at[5 + size + k], member=other)
        for k, other in enumerate(others)
    ]
    for copy in pooled_own:
        copy.start()
    start_halo(pooled_halo)
    ring.stage(0, 4)

    for part in range(3):
        here = slice(part * rows, (part + 1) * rows)
        offset = (0, -rows, rows)[part]
        key_row = lax.broadcasted_iota(jnp.int32, (rows, rows), 0) + offset
        query_row = lax.broadcasted_iota(jnp.int32, (rows, rows), 1)
        column = key_row + region * rows
        allowed = (
            (jnp.abs(key_row - query_row) <= reach_ref[...])
            & (column >= 0)
            & (column < node_total)
        )
        bias[here, :] = jnp.where(allowed, 0.0, -1e30)

    def embed_rows(part):
        here = slice(part * rows, (part + 1) * rows)
        embedded = lax.dot_general(
            pooled[:, here], embed[...], (((0,), (0,)), ((), ())),
            preferred_element_type=jnp.float32,
        )
        begin = embedded + perturb[here, :].astype(jnp.float32)
        normed[here, :] = layer_norm(begin, gains_ref[0:1, :]).astype(jnp.bfloat16)
        return begin

    for copy in pooled_own:
        copy.wait_recv()
    own_perturb.wait()
    mid_out[...] = embed_rows(0)
    load_qkv.wait()
    tile = 256

    def project(first, last, column):
        return jnp.dot(
            normed[first:last, :],
            qkv_w[:, pl.ds(pl.multiple_of(column * tile, tile), tile)],
            preferred_element_type=jnp.float32,
        ).astype(jnp.bfloat16)

    tiles = width // tile

    def own_tile(index, carry):
        place = pl.ds(pl.multiple_of(index * tile, tile), tile)
        query[:, place] = project(0, rows, index) * jnp.bfloat16(HEAD_DIM ** (-0.5))
        keys[0:rows, place] = project(0, rows, tiles + index)
        values_t[place, 0:rows] = project(0, rows, 2 * tiles + index).T
        return carry

    lax.fori_loop(0, tiles, own_tile, 0)
    ring.stage(1, 4)

    take_halo(pooled_halo)
    edges = pooled.at[mine, pl.ds(rows, 2 * rows)]
    pooled_edges = [
        copy_to(edges, edges, sems.at[5 + 2 * size + k], sems.at[5 + 3 * size + k], member=other)
        for k, other in enumerate(others)
    ]
    for copy in pooled_edges:
        copy.start()
    take_halo(perturb_halo)
    for copy in pooled_edges:
        copy.wait_recv()
    embed_rows(1)
    embed_rows(2)

    def edge_tile(index, carry):
        place = pl.ds(pl.multiple_of(index * tile, tile), tile)
        keys[rows:, place] = project(rows, 3 * rows, tiles + index)
        values_t[place, rows:] = project(rows, 3 * rows, 2 * tiles + index).T
        return carry

    lax.fori_loop(0, tiles, edge_tile, 0)
    ring.stage(2, 4)

    pair = 2 * HEAD_DIM
    lane = lax.broadcasted_iota(jnp.int32, (rows, pair), 1)

    def attend(index, carry):
        place = pl.ds(pl.multiple_of(index * pair, pair), pair)
        both = query[:, place]
        key_pair = keys[:, place]
        for head in range(2):
            chosen = (lane < HEAD_DIM) if head == 0 else (lane >= HEAD_DIM)
            scores = times_rows(key_pair, jnp.where(chosen, both, jnp.zeros_like(both)))
            scores = scores + bias[...]
            highest = jnp.max(scores, axis=0, keepdims=True)
            weights = jnp.exp(scores - highest)
            total = jnp.sum(weights, axis=0, keepdims=True)
            lines = pl.ds(pl.multiple_of(index * pair + head * HEAD_DIM, HEAD_DIM), HEAD_DIM)
            blended = jnp.dot(
                values_t[lines, :], weights.astype(jnp.bfloat16),
                preferred_element_type=jnp.float32,
            )
            attended_t[lines, :] = (blended * (1.0 / total)).astype(jnp.bfloat16)
        return carry

    pairs = width // pair
    lax.fori_loop(0, pairs // 2, attend, 0)
    ring.stage(3, 4)
    lax.fori_loop(pairs // 2, pairs, attend, 0)

    load_out.wait()
    middle = mid_out[...] + lax.dot_general(
        attended_t[...], out_w[...], (((0,), (0,)), ((), ())), preferred_element_type=jnp.float32
    )
    mid_out[...] = middle
    norm_out[...] = layer_norm(middle, gains_ref[1:2, :]).astype(jnp.bfloat16)

    ring.finish()
    for copy in pooled_own + pooled_edges:
        copy.wait_send()
    for pair_of in (state_halo, perturb_halo, pooled_halo):
        end_halo(pair_of)


def front(share, slots, uses, reach, embed_weight, gains, perturb, qkv_weight, out_weight, up, down):
    count = lax.axis_size("node")
    size = lax.axis_size("member")
    channels, grid_dev = share.shape
    rows, width = perturb.shape
    quarter = up.shape[1] // size
    kind = jnp.bfloat16
    sem = pltpu.SemaphoreType.DMA
    vmem = pl.BlockSpec(memory_space=pltpu.VMEM)
    anywhere = pl.BlockSpec(memory_space=pl.ANY)
    hops = count - 1 - (count - 1) // 2
    wide = size * channels
    return pl.pallas_call(
        functools.partial(front_kernel, count, size),
        out_shape=(
            jax.ShapeDtypeStruct((up.shape[0] * count, quarter), kind),
            jax.ShapeDtypeStruct((down.shape[0] * count, quarter), kind),
            jax.ShapeDtypeStruct((rows, width), jnp.float32),
            jax.ShapeDtypeStruct((rows, width), kind),
        ),
        in_specs=[vmem] * 6 + [anywhere] * 5,
        out_specs=(vmem,) * 4,
        scratch_shapes=[
            pltpu.VMEM((channels, 3 * grid_dev), kind),
            pltpu.VMEM((3 * grid_dev, rows), kind),
            pltpu.VMEM((wide, 3 * rows), kind),
            pltpu.VMEM((3 * rows, width), kind),
            pltpu.VMEM((wide, width), kind),
            pltpu.VMEM((3 * rows, width), kind),
            pltpu.VMEM(qkv_weight.shape, kind),
            pltpu.VMEM(out_weight.shape, kind),
            pltpu.VMEM((rows, width), kind),
            pltpu.VMEM((3 * rows, width), kind),
            pltpu.VMEM((width, 3 * rows), kind),
            pltpu.VMEM((3 * rows, rows), jnp.float32),
            pltpu.VMEM((width, rows), kind),
            sem((5 + 4 * size,)),
            sem((3, 2)),
            sem((3, 2)),
            sem((2, 2, hops)),
            sem((2, 2, hops)),
        ],
        compiler_params=pltpu.CompilerParams(collective_id=2, has_side_effects=True),
        cost_estimate=pl.CostEstimate(flops=10**10, bytes_accessed=10**7, transcendentals=0),
        name="front",
    )(share, slots, uses, reach, embed_weight, gains, perturb, qkv_weight, out_weight, up, down)


def peers_of(size):
    me = lax.axis_index("member")
    mate = me + 1 - 2 * lax.rem(me, 2)
    ahead = [lax.rem(me + 2 * k, size) for k in range(1, size // 2)]
    behind = [lax.rem(me + size - 2 * k, size) for k in range(1, size // 2)]
    return me, mate, ahead, behind


def greet(mate, ahead, behind):
    barrier = pltpu.get_barrier_semaphore()
    others = [mate] + ahead + behind
    for other in others:
        pl.semaphore_signal(
            barrier, inc=1, device_id={"member": other}, device_id_type=pl.DeviceIdType.MESH
        )
    pl.semaphore_wait(barrier, len(others))


def remote(source, target, send_sem, recv_sem, member):
    return pltpu.make_async_remote_copy(
        src_ref=source,
        dst_ref=target,
        send_sem=send_sem,
        recv_sem=recv_sem,
        device_id={"member": member},
        device_id_type=pl.DeviceIdType.MESH,
    )


def rows_of(index, rows, step, chunk):
    return pl.ds(pl.multiple_of(index * rows + step * chunk, chunk), chunk)


def gather_kernel(size, chunks, x_ref, o_ref, sib_s, sib_r, out_s, out_r, fwd_s, fwd_r, own_sem):
    me, mate, ahead, behind = peers_of(size)
    rows = x_ref.shape[0]
    chunk = rows // chunks
    greet(mate, ahead, behind)
    sends = []
    for step in range(chunks):
        for k, peer in enumerate(ahead):
            copy = remote(
                x_ref.at[pl.ds(step * chunk, chunk)],
                o_ref.at[rows_of(me, rows, step, chunk)],
                out_s.at[k, step],
                out_r.at[k, step],
                peer,
            )
            copy.start()
            sends.append(copy)
    to_mate = remote(x_ref, o_ref.at[rows_of(me, rows, 0, rows)], sib_s, sib_r, mate)
    to_mate.start()
    own = pltpu.make_async_copy(x_ref, o_ref.at[rows_of(me, rows, 0, rows)], own_sem)
    own.start()
    forwards = []
    for step in range(chunks):
        for k in range(len(ahead)):
            sends[step * len(ahead) + k].wait_recv()
            place = rows_of(behind[k], rows, step, chunk)
            copy = remote(
                o_ref.at[place], o_ref.at[place], fwd_s.at[k, step], fwd_r.at[k, step], mate
            )
            copy.start()
            forwards.append(copy)
    own.wait()
    to_mate.wait()
    for copy in forwards:
        copy.wait()
    for copy in sends:
        copy.wait_send()


def member_gather(entries, size):
    rows, width = entries.shape
    chunks = 4
    far = size // 2 - 1
    sem = pltpu.SemaphoreType.DMA
    return pl.pallas_call(
        functools.partial(gather_kernel, size, chunks),
        out_shape=jax.ShapeDtypeStruct((size * rows, width), entries.dtype),
        in_specs=[pl.BlockSpec(memory_space=pltpu.VMEM)],
        out_specs=pl.BlockSpec(memory_space=pltpu.VMEM),
        scratch_shapes=[sem, sem, sem((far, chunks)), sem((far, chunks)), sem((far, chunks)), sem((far, chunks)), sem],
        compiler_params=pltpu.CompilerParams(collective_id=0, has_side_effects=True),
        cost_estimate=pl.CostEstimate(flops=10**10, bytes_accessed=10**6, transcendentals=0),
        name="member_gather",
    )(entries)


def scatter_kernel(
    size, chunks, p_ref, o_ref, own_in, fwd_in, acc, far_in, own_s, own_r, fwd_s, fwd_r, far_s, far_r
):
    me, mate, ahead, behind = peers_of(size)
    rows = o_ref.shape[0]
    chunk = rows // chunks
    greet(mate, ahead, behind)
    relayed = []
    for step in range(chunks):
        here = pl.ds(step * chunk, chunk)
        for k, peer in enumerate(ahead):
            beside = peer + 1 - 2 * lax.rem(peer, 2)
            copy = remote(
                p_ref.at[rows_of(beside, rows, step, chunk)],
                fwd_in.at[k, here],
                fwd_s.at[k, step],
                fwd_r.at[k, step],
                mate,
            )
            copy.start()
            relayed.append(copy)
    to_mate = remote(p_ref.at[rows_of(mate, rows, 0, rows)], own_in, own_s, own_r, mate)
    to_mate.start()
    sends = []
    for step in range(chunks):
        here = pl.ds(step * chunk, chunk)
        for k, peer in enumerate(ahead):
            relayed[step * len(ahead) + k].wait_recv()
            acc[k, here] = (
                p_ref[rows_of(peer, rows, step, chunk), :].astype(jnp.float32)
                + fwd_in[k, here].astype(jnp.float32)
            ).astype(acc.dtype)
            copy = remote(
                acc.at[k, here], far_in.at[k, here], far_s.at[k, step], far_r.at[k, step], peer
            )
            copy.start()
            sends.append(copy)
    to_mate.wait()
    for step in range(chunks):
        here = pl.ds(step * chunk, chunk)
        total = p_ref[rows_of(me, rows, step, chunk), :].astype(jnp.float32) + own_in[
            here, :
        ].astype(jnp.float32)
        for k in range(len(ahead)):
            sends[step * len(ahead) + k].wait_recv()
            total = total + far_in[k, here].astype(jnp.float32)
        o_ref[here, :] = total
    for copy in relayed + sends:
        copy.wait_send()


def member_scatter(partial, size):
    rows, width = partial.shape[0] // size, partial.shape[1]
    chunks = 4
    far = size // 2 - 1
    kind = partial.dtype
    sem = pltpu.SemaphoreType.DMA
    return pl.pallas_call(
        functools.partial(scatter_kernel, size, chunks),
        out_shape=jax.ShapeDtypeStruct((rows, width), jnp.float32),
        in_specs=[pl.BlockSpec(memory_space=pltpu.VMEM)],
        out_specs=pl.BlockSpec(memory_space=pltpu.VMEM),
        scratch_shapes=[
            pltpu.VMEM((rows, width), kind),
            pltpu.VMEM((far, rows, width), kind),
            pltpu.VMEM((far, rows, width), kind),
            pltpu.VMEM((far, rows, width), kind),
            sem, sem, sem((far, chunks)), sem((far, chunks)), sem((far, chunks)), sem((far, chunks)),
        ],
        compiler_params=pltpu.CompilerParams(collective_id=1, has_side_effects=True),
        cost_estimate=pl.CostEstimate(flops=10**10, bytes_accessed=10**6, transcendentals=0),
        name="member_scatter",
    )(partial)


def per_device(
    gridpoint_state,
    grid_truth,
    encoder_slots,
    encoder_count,
    node_reach,
    decoder_slots,
    member_perturb,
    embed_weight,
    norm_gains,
    qkv_weight,
    out_weight,
    up_weight,
    down_weight,
    head_weight,
):
    region = lax.axis_index("node")
    ensemble_size = lax.axis_size("member")
    member_index = lax.axis_index("member")
    channels, grid_dev = gridpoint_state.shape
    node_dev = encoder_slots.shape[0]
    share = -(-channels // (16 * ensemble_size)) * 16
    extra = share * ensemble_size - channels
    state_wide = jnp.pad(gridpoint_state, ((0, extra), (0, 0)))
    state_share = lax.dynamic_slice_in_dim(state_wide, member_index * share, share, 0)
    slots = encoder_slots - (region - 1) * grid_dev
    live = jnp.arange(slots.shape[1], dtype=jnp.int32)[None, :] < encoder_count[:, None]
    slots = jnp.where(live, slots, -1).T
    near = count_slots(decoder_slots - (region - 1) * node_dev, None, 3 * node_dev)
    up_whole, down_whole, hidden_mid, normed_mid = front(
        state_share,
        slots,
        encoder_count[None, :].astype(jnp.float32),
        node_reach[None, :],
        embed_weight,
        norm_gains,
        member_perturb[0],
        qkv_weight,
        out_weight,
        up_weight,
        down_weight,
    )
    normed_all = member_gather(normed_mid, ensemble_size)
    upper = jnp.dot(normed_all, up_whole, preferred_element_type=jnp.float32)
    active_all = jax.nn.gelu(upper).astype(jnp.bfloat16)
    partial_terms = times_rows(active_all, down_whole)
    lowered = member_scatter(partial_terms.astype(jnp.bfloat16), ensemble_size)
    final = layer_norm(hidden_mid + lowered, norm_gains[2]).astype(jnp.bfloat16)

    variables = head_weight.shape[1]
    padded = -(-variables // 16) * 16
    head_wide = jnp.pad(head_weight, ((0, 0), (0, padded - variables)))
    node_terms = lax.dot_general(
        head_wide, final, (((0,), (1,)), ((), ())), preferred_element_type=jnp.float32
    ).astype(jnp.bfloat16)
    node_terms = with_halo(node_terms, 1, node_dev)
    every_terms = lax.all_gather(node_terms, "member", axis=0, tiled=True)
    state_delta = times_rows(every_terms, near) / decoder_slots.shape[1]
    state_delta = state_delta.reshape(ensemble_size, padded, grid_dev)[:, :variables]
    whole_ensemble = gridpoint_state[:variables].astype(jnp.float32)[None] + state_delta
    predicted_field = lax.dynamic_index_in_dim(whole_ensemble, member_index, 0, keepdims=False)
    observed_field = grid_truth.astype(jnp.float32)
    pairwise_scale = 1.0 / (ensemble_size * (ensemble_size - 1))
    pairwise_sum = jnp.zeros_like(predicted_field)
    for other_member in range(ensemble_size):
        pairwise_sum = pairwise_sum + score_gradient(predicted_field - whole_ensemble[other_member])
    step_output = (
        score_gradient(predicted_field - observed_field) / ensemble_size
        - pairwise_sum * pairwise_scale
    )
    return step_output[None]


def solution(mesh):
    placed = (
        P(None, "node"),
        P(None, "node"),
        P("node", None),
        P("node"),
        P("node"),
        P("node", None),
        P("member", "node", None),
        P(),
        P(),
        P(),
        P(),
        P("node", None),
        P("node", None),
        P(),
    )

    return jax.shard_map(
        per_device, mesh=mesh, in_specs=placed, out_specs=P("member", None, "node"), check_vma=False
    )
```
